8 devices in a mesh: data: 1 (over z), dap: 8 (over y, x, core).
Axes of the slice: x: 2, y: 2, z: 1, core: 2. Of those that a mesh axis runs over, the one named last changes fastest.
Arguments:
- pair_rep: bfloat16 [4, 768, 768, 128], P('data', 'dap')
- pair_mask: int32 [4, 768, 768], P('data', 'dap')
- norm_gain: bfloat16 [2, 128], replicated
- norm_bias: bfloat16 [2, 128], replicated
- w_proj: bfloat16 [2, 128, 512], replicated
- w_gate: bfloat16 [2, 128, 128], replicated
- hid_gain: bfloat16 [2, 128], replicated
- hid_bias: bfloat16 [2, 128], replicated
- w_out: bfloat16 [2, 128, 128], replicated
Outputs:
- output: bfloat16 [4, 768, 768, 128], P('data', None, 'dap')
All inputs are finite; a program needn't handle non-finite values.
Results may differ from the reference program's by a relative error of at most 0.00637242.
Values are sent between devices in bfloat16 or wider.
A program may use at most 1 GiB of HBM per device.

```python
import jax
import jax.numpy as jnp
from jax import lax

NUM_CROPS = 4
N_RES = 768
C_PAIR = 128
C_HIDDEN = 128
LN_EPS = 1e-5
BLOCK_ROWS = min(N_RES, 64)


def setup_inputs(seed: int = 0, part: int = 0) -> dict:
    key_list = jax.random.split(jax.random.key(seed), 8)
    part_key = jax.random.fold_in(key_list[0], part)
    key_pair, key_keep, key_len = jax.random.split(part_key, 3)
    pair_vals = jax.random.normal(key_pair, (NUM_CROPS, N_RES, N_RES, C_PAIR), jnp.float32)
    keep_res = jax.random.randint(key_keep, (NUM_CROPS, N_RES), 0, 16) != 0
    pad_len = jax.random.randint(key_len, (NUM_CROPS, 1), 0, N_RES // 8 + 1)
    res_valid = (keep_res & (jnp.arange(N_RES)[None, :] < N_RES - pad_len)).astype(jnp.int32)
    pair_mask = res_valid[:, :, None] * res_valid[:, None, :]
    norm_gain = 1.0 + 0.3 * jax.random.normal(key_list[1], (2, C_PAIR), jnp.float32)
    norm_bias = 0.3 * jax.random.normal(key_list[2], (2, C_PAIR), jnp.float32)
    w_proj = jax.random.normal(key_list[3], (2, C_PAIR, 4 * C_HIDDEN), jnp.float32) * C_PAIR ** -0.5
    w_gate = jax.random.normal(key_list[4], (2, C_PAIR, C_PAIR), jnp.float32) * C_PAIR ** -0.5
    hid_gain = 1.0 + 0.3 * jax.random.normal(key_list[5], (2, C_HIDDEN), jnp.float32)
    hid_bias = 0.3 * jax.random.normal(key_list[6], (2, C_HIDDEN), jnp.float32)
    w_out = jax.random.normal(key_list[7], (2, C_HIDDEN, C_PAIR), jnp.float32) * C_HIDDEN ** -0.5
    return {
        'pair_rep': pair_vals.astype(jnp.bfloat16),
        'pair_mask': pair_mask,
        'norm_gain': norm_gain.astype(jnp.bfloat16),
        'norm_bias': norm_bias.astype(jnp.bfloat16),
        'w_proj': w_proj.astype(jnp.bfloat16),
        'w_gate': w_gate.astype(jnp.bfloat16),
        'hid_gain': hid_gain.astype(jnp.bfloat16),
        'hid_bias': hid_bias.astype(jnp.bfloat16),
        'w_out': w_out.astype(jnp.bfloat16),
    }


def layer_norm(values, gain_vec, bias_vec):
    centred = values - jnp.mean(values, axis=-1, keepdims=True)
    var_val = jnp.mean(centred * centred, axis=-1, keepdims=True)
    return centred * lax.rsqrt(var_val + LN_EPS) * gain_vec.astype(jnp.float32) + bias_vec.astype(jnp.float32)


def project(pair_rows, mask_rows, norm_gain, norm_bias, w_proj):
    normed = layer_norm(pair_rows.astype(jnp.float32), norm_gain, norm_bias).astype(jnp.bfloat16)
    proj_all = jnp.dot(normed.reshape(-1, C_PAIR), w_proj, preferred_element_type=jnp.float32)
    proj_all = proj_all.reshape(BLOCK_ROWS, N_RES, 4, C_HIDDEN)
    mask_f = mask_rows.astype(jnp.float32)[:, :, None]
    left_proj = (mask_f * jax.nn.sigmoid(proj_all[:, :, 1]) * proj_all[:, :, 0]).astype(jnp.bfloat16)
    right_proj = (mask_f * jax.nn.sigmoid(proj_all[:, :, 3]) * proj_all[:, :, 2]).astype(jnp.bfloat16)
    return left_proj, right_proj


def finish(pair_rows, tri_sum, norm_gain, norm_bias, w_gate, hid_gain, hid_bias, w_out):
    normed = layer_norm(pair_rows.astype(jnp.float32), norm_gain, norm_bias).astype(jnp.bfloat16)
    gate_val = jax.nn.sigmoid(jnp.dot(normed.reshape(-1, C_PAIR), w_gate, preferred_element_type=jnp.float32))
    tri_round = tri_sum.astype(jnp.bfloat16).astype(jnp.float32)
    hid_norm = layer_norm(tri_round, hid_gain, hid_bias).astype(jnp.bfloat16)
    out_proj = jnp.dot(hid_norm.reshape(-1, C_HIDDEN), w_out, preferred_element_type=jnp.float32)
    new_rows = pair_rows.astype(jnp.float32) + (gate_val * out_proj).reshape(BLOCK_ROWS, N_RES, C_PAIR)
    return new_rows.astype(jnp.bfloat16)


def tri_update(pair_grid, mask_grid, weights, layer_idx, incoming):
    norm_gain, norm_bias, w_proj, w_gate, hid_gain, hid_bias, w_out = [w_arr[layer_idx] for w_arr in weights]
    n_blocks = N_RES // BLOCK_ROWS

    def proj_block(blk_idx):
        row_start = blk_idx * BLOCK_ROWS
        pair_rows = lax.dynamic_slice_in_dim(pair_grid, row_start, BLOCK_ROWS, 0)
        mask_rows = lax.dynamic_slice_in_dim(mask_grid, row_start, BLOCK_ROWS, 0)
        return project(pair_rows, mask_rows, norm_gain, norm_bias, w_proj)

    left_proj, right_proj = lax.map(proj_block, jnp.arange(n_blocks))
    left_proj = left_proj.reshape(N_RES, N_RES, C_HIDDEN)
    right_all = right_proj.reshape(N_RES, N_RES, C_HIDDEN).astype(jnp.float32)

    def out_block(blk_idx):
        row_start = blk_idx * BLOCK_ROWS
        pair_rows = lax.dynamic_slice_in_dim(pair_grid, row_start, BLOCK_ROWS, 0)
        if incoming:
            left_blk = lax.dynamic_slice_in_dim(left_proj, row_start, BLOCK_ROWS, 1).astype(jnp.float32)
            tri_sum = jnp.einsum('kic,kjc->ijc', left_blk, right_all)
        else:
            left_blk = lax.dynamic_slice_in_dim(left_proj, row_start, BLOCK_ROWS, 0).astype(jnp.float32)
            tri_sum = jnp.einsum('ikc,jkc->ijc', left_blk, right_all)
        return finish(pair_rows, tri_sum, norm_gain, norm_bias, w_gate, hid_gain, hid_bias, w_out)

    new_grid = lax.map(out_block, jnp.arange(n_blocks))
    return new_grid.reshape(N_RES, N_RES, C_PAIR)


def reference(pair_rep, pair_mask, norm_gain, norm_bias, w_proj, w_gate, hid_gain, hid_bias, w_out):
    weights = (norm_gain, norm_bias, w_proj, w_gate, hid_gain, hid_bias, w_out)

    def per_crop(crop_item):
        pair_grid, mask_grid = crop_item
        mid_grid = tri_update(pair_grid, mask_grid, weights, 0, False)
        return tri_update(mid_grid, mask_grid, weights, 1, True)

    return lax.map(per_crop, (pair_rep, pair_mask))
```

```python
import jax
import jax.numpy as jnp
from jax import lax
from jax.experimental import pallas as pl
from jax.experimental.pallas import tpu as pltpu
from jax.sharding import PartitionSpec as P


LN_EPS = 1e-5
ROWS = 16
VMEM = 63 * 1024 * 1024
N_DEV = 8
N_CHIP = 4
SAME_CORE = [[0, 2, 4, 6], [1, 3, 5, 7]]
F32 = jnp.float32
BF16 = jnp.bfloat16


def norm(v, axis):
    centred = v - jnp.mean(v, axis=axis, keepdims=True)
    var_val = jnp.mean(centred * centred, axis=axis, keepdims=True)
    return centred * lax.rsqrt(var_val + LN_EPS)


def nt_dot(lhs, rhs):
    return lax.dot_general(lhs, rhs, (((1,), (1,)), ((), ())), preferred_element_type=F32)


def tn_dot(lhs, rhs):
    return lax.dot_general(lhs, rhs, (((0,), (0,)), ((), ())), preferred_element_type=F32)


def proj_row(x, wt):
    q = nt_dot(wt, x)
    hid = q.shape[0] // 4
    left = (jnp.tanh(q[hid:2 * hid]) + 1.0) * q[:hid]
    right = (jnp.tanh(q[3 * hid:]) + 1.0) * q[2 * hid:3 * hid]
    return left, right


def row_norm(z, gain, bias):
    return (norm(z.astype(F32), -1) * gain + bias).astype(BF16)


def channel_major(rows, mask):
    return jnp.swapaxes(jnp.stack(rows), 0, 1).astype(BF16) * mask[None]


def put_ab(lefts, rights, mask, refs):
    for rows, (part, *outs) in ((lefts, (0, *refs)), (rights, (1, *refs))):
        block = channel_major(rows, mask)
        start = 0
        for out in outs:
            size = out.shape[1]
            out[part] = block[start:start + size]
            start += size


def proj_kernel(z_ref, m_ref, gain_ref, bias_ref, wt_ref, a_ref, b_ref):
    gain, bias = gain_ref[...].astype(F32), bias_ref[...].astype(F32)
    wt = wt_ref[...]
    lefts, rights = [], []
    for i in range(z_ref.shape[0]):
        x = row_norm(z_ref[i], gain, bias)
        left, right = proj_row(x, wt)
        lefts.append(left)
        rights.append(right)
    mask = m_ref[...].astype(F32).astype(BF16)
    a_ref[...] = channel_major(lefts, mask)
    b_ref[...] = channel_major(rights, mask)


def hidden_rows(tri, hgain, hbias):
    h = norm(tri.astype(F32), 0) * hgain[...].astype(F32) + hbias[...].astype(F32)
    return jnp.swapaxes(h, 0, 1).astype(BF16)


def update_row(z, h_row, gain, bias, w_gate, w_out):
    x = row_norm(z, gain, bias)
    gate = jnp.tanh(jnp.dot(x, w_gate, preferred_element_type=F32)) + 1.0
    return (z.astype(F32) + gate * tn_dot(h_row, w_out)).astype(BF16)


def mid_kernel(z_ref, t_ref, m_ref, gain_ref, bias_ref, wg_ref, hg_ref, hb_ref, wo_ref,
               gain2_ref, bias2_ref, wt_ref, z1_ref, keep_ref, send_ref):
    gain, bias = gain_ref[...].astype(F32), bias_ref[...].astype(F32)
    gain2, bias2 = gain2_ref[...].astype(F32), bias2_ref[...].astype(F32)
    w_gate, w_out, wt = wg_ref[...], wo_ref[...], wt_ref[...]
    h = hidden_rows(t_ref[...], hg_ref, hb_ref)
    lefts, rights = [], []
    for i in range(z_ref.shape[0]):
        z1 = update_row(z_ref[i], h[i], gain, bias, w_gate, w_out)
        z1_ref[i] = z1
        left, right = proj_row(row_norm(z1, gain2, bias2), wt)
        lefts.append(left)
        rights.append(right)
    put_ab(lefts, rights, m_ref[...].astype(F32).astype(BF16), (keep_ref, send_ref))


def last_kernel(z_ref, tk_ref, tr_ref, gain_ref, bias_ref, wg_ref, hg_ref, hb_ref, wo_ref, out_ref):
    gain, bias = gain_ref[...].astype(F32), bias_ref[...].astype(F32)
    w_gate, w_out = wg_ref[...], wo_ref[...]
    tri = jnp.concatenate([tk_ref[...], tr_ref[...]], axis=0)
    h = hidden_rows(tri, hg_ref, hb_ref)
    for i in range(z_ref.shape[0]):
        z2 = update_row(z_ref[i], h[i], gain, bias, w_gate, w_out)
        out_ref[:, i] = z2.reshape(out_ref.shape[0], -1, z2.shape[-1])


def tri_out_kernel(pos_ref, *refs):
    left, own, par, outs = refs[0:4], refs[4:8], refs[8:12], refs[12:16]
    rhs = refs[16]
    chip, core = pos_ref[0], pos_ref[1]
    rows = left[0].shape[1]
    for c in range(left[0].shape[0]):
        for r in range(N_CHIP):
            base = 2 * jnp.bitwise_xor(chip, r)
            rhs[c, pl.ds(pl.multiple_of((base + core) * rows, 32), rows), :] = own[r][c]
            rhs[c, pl.ds(pl.multiple_of((base + 1 - core) * rows, 32), rows), :] = par[r][c]
        lhs = jnp.concatenate([left[r][c] for r in range(N_CHIP)], axis=0)
        tri = nt_dot(lhs, rhs[c]).astype(BF16)
        for r in range(N_CHIP):
            outs[r][c] = tri[r * rows:(r + 1) * rows]


def tri_in_kernel(pos_ref, *refs):
    own, par, keep, send = refs[0:4], refs[4:8], refs[8:12], refs[12:16]
    buf = refs[16]
    chip, core = pos_ref[0], pos_ref[1]
    rows = keep[0].shape[1]
    for c in range(keep[0].shape[0]):
        lhs = jnp.concatenate([ref[0, c] for ref in own + par], axis=0)
        rhs = jnp.concatenate([ref[1, c] for ref in own + par], axis=0)
        buf[c] = tn_dot(lhs, rhs).astype(BF16)
        for r in range(N_CHIP):
            base = 2 * jnp.bitwise_xor(chip, r)
            keep[r][c] = buf[c, pl.ds(pl.multiple_of((base + core) * rows, 32), rows), :]
            send[r][c] = buf[c, pl.ds(pl.multiple_of((base + 1 - core) * rows, 32), rows), :]


def whole(arr):
    return pl.BlockSpec(arr.shape, lambda *_: (0,) * arr.ndim)


def params(limit=VMEM):
    return pltpu.CompilerParams(vmem_limit_bytes=limit)


def proj_call(z, mask, gain, bias, wt):
    rows, cols, chan = z.shape
    hid = wt.shape[0] // 4
    spec = pl.BlockSpec((hid, ROWS, cols), lambda i: (0, i, 0))
    shape = jax.ShapeDtypeStruct((hid, rows, cols), BF16)
    pts = rows * cols
    return pl.pallas_call(
        proj_kernel, grid=(rows // ROWS,), name='proj',
        in_specs=[pl.BlockSpec((ROWS, cols, chan), lambda i: (i, 0, 0)), pl.BlockSpec((ROWS, cols), lambda i: (i, 0)),
                  whole(gain), whole(bias), whole(wt)],
        out_specs=[spec, spec], out_shape=[shape, shape], compiler_params=params(),
        cost_estimate=pl.CostEstimate(flops=2 * pts * chan * hid * 4 * 4, bytes_accessed=pts * chan * 6,
                                      transcendentals=0),
    )(z, mask, gain, bias, wt)


def mid_call(z, tri, mask, upd, nxt):
    rows, cols, chan = z.shape
    hid = tri.shape[0]
    ab_spec = pl.BlockSpec((2, hid // 2, ROWS, cols), lambda i: (0, 0, i, 0))
    ab_shape = jax.ShapeDtypeStruct((2, hid // 2, rows, cols), BF16)
    z_spec = pl.BlockSpec((ROWS, cols, chan), lambda i: (i, 0, 0))
    pts = rows * cols
    return pl.pallas_call(
        mid_kernel, grid=(rows // ROWS,), name='mid',
        in_specs=[z_spec, pl.BlockSpec((hid, ROWS, cols), lambda i: (0, i, 0)),
                  pl.BlockSpec((ROWS, cols), lambda i: (i, 0))] + [whole(w) for w in upd + nxt],
        out_specs=[z_spec, ab_spec, ab_spec],
        out_shape=[jax.ShapeDtypeStruct(z.shape, BF16), ab_shape, ab_shape], compiler_params=params(),
        cost_estimate=pl.CostEstimate(flops=2 * pts * chan * hid * 6 * 4, bytes_accessed=pts * chan * 10,
                                      transcendentals=0),
    )(z, tri, mask, *upd, *nxt)


def last_call(z, keep, recv, upd):
    rows, cols, chan = z.shape
    half = keep.shape[0]
    t_spec = pl.BlockSpec((half, ROWS, cols), lambda i: (0, i, 0))
    pts = rows * cols
    return pl.pallas_call(
        last_kernel, grid=(rows // ROWS,), name='last',
        in_specs=[pl.BlockSpec((ROWS, cols, chan), lambda i: (i, 0, 0)), t_spec, t_spec] + [whole(w) for w in upd],
        out_specs=pl.BlockSpec((N_DEV, ROWS, cols // N_DEV, chan), lambda i: (0, i, 0, 0)),
        out_shape=jax.ShapeDtypeStruct((N_DEV, rows, cols // N_DEV, chan), BF16), compiler_params=params(),
        cost_estimate=pl.CostEstimate(flops=2 * pts * chan * half * 4 * 4, bytes_accessed=pts * chan * 6,
                                      transcendentals=0),
    )(z, keep, recv, *upd)


def tri_out_call(pos, left, own, par, chans=2):
    hid, rows, cols = left[0].shape
    spec = pl.BlockSpec((chans, rows, cols), lambda c, pos: (c, 0, 0))
    shape = jax.ShapeDtypeStruct((hid, rows, cols), BF16)
    grid = pltpu.PrefetchScalarGridSpec(
        num_scalar_prefetch=1, grid=(hid // chans,), in_specs=[spec] * 12, out_specs=[spec] * 4,
        scratch_shapes=[pltpu.VMEM((chans, N_DEV * rows, cols), BF16)])
    return pl.pallas_call(
        tri_out_kernel, grid_spec=grid, out_shape=[shape] * 4, name='tri_out', compiler_params=params(),
        cost_estimate=pl.CostEstimate(flops=2 * hid * 4 * rows * cols * cols, bytes_accessed=hid * rows * cols * 32,
                                      transcendentals=0),
    )(pos, *left, *own, *par)


def tri_in_call(pos, own, par, chans=2):
    _, half, rows, cols = own[0].shape
    in_spec = pl.BlockSpec((2, chans, rows, cols), lambda c, pos: (0, c, 0, 0))
    spec = pl.BlockSpec((chans, rows, cols), lambda c, pos: (c, 0, 0))
    shape = jax.ShapeDtypeStruct((half, rows, cols), BF16)
    grid = pltpu.PrefetchScalarGridSpec(
        num_scalar_prefetch=1, grid=(half // chans,), in_specs=[in_spec] * 8, out_specs=[spec] * 8,
        scratch_shapes=[pltpu.VMEM((chans, N_DEV * rows, cols), BF16)])
    outs = pl.pallas_call(
        tri_in_kernel, grid_spec=grid, out_shape=[shape] * 8, name='tri_in', compiler_params=params(),
        cost_estimate=pl.CostEstimate(flops=2 * half * 8 * rows * cols * cols, bytes_accessed=half * rows * cols * 48,
                                      transcendentals=0),
    )(pos, *own, *par)
    return outs[:4], outs[4:]


def place_kernel(*refs):
    refs[-1][0, 0] = refs[0][0]


def place_call(part, r, out):
    shape = jax.ShapeDtypeStruct((N_CHIP, N_DEV) + part.shape[1:], part.dtype)
    args, specs, alias = [part], [pl.BlockSpec((1,) + part.shape[1:], lambda d: (d, 0, 0, 0))], {}
    if out is not None:
        args.append(out)
        specs.append(pl.BlockSpec(memory_space=pl.ANY))
        alias = {1: 0}
    return pl.pallas_call(
        place_kernel, grid=(N_DEV,), name='place', in_specs=specs, out_shape=shape, input_output_aliases=alias,
        out_specs=pl.BlockSpec((1, 1) + part.shape[1:],
                               lambda d: (d // 2, 2 * jnp.bitwise_xor(d // 2, r) + d % 2, 0, 0, 0)),
        compiler_params=params(),
    )(*args)


def swap(arr, bits):
    return lax.ppermute(arr, 'dap', [(d, d ^ bits) for d in range(N_DEV)])


def solution(mesh):
    def body(pair, mask, norm_gain, norm_bias, w_proj, w_gate, hid_gain, hid_bias, w_out):
        me = lax.axis_index('dap')
        chip, core = me // 2, me % 2
        pos = jnp.stack([chip, core]).astype(jnp.int32)
        half = hid_gain.shape[1] // 2

        def col(v):
            return v.reshape(-1, 1, 1)

        def rolled(v, axis):
            return jnp.roll(v, -half * core, axis)

        gain, bias = norm_gain[:, None, :], norm_bias[:, None, :]
        wt1 = 0.5 * w_proj[0].T
        wt2 = rolled(0.5 * w_proj[1].T.reshape(4, 2 * half, -1), 1).reshape(8 * half, -1)
        upd1 = (gain[0], bias[0], 0.5 * w_gate[0], col(hid_gain[0]), col(hid_bias[0]), 0.5 * w_out[0])
        upd2 = (gain[1], bias[1], 0.5 * w_gate[1], col(rolled(hid_gain[1], 0)), col(rolled(hid_bias[1], 0)),
                rolled(0.5 * w_out[1], 0))

        def pick(arr, r):
            return lax.dynamic_index_in_dim(arr, jnp.bitwise_xor(chip, r), 0, False)

        masks = lax.all_to_all(mask, 'dap', 0, 0, tiled=True, axis_index_groups=SAME_CORE)
        ms = [pick(masks, r) for r in range(N_CHIP)]
        zs = [None] * N_CHIP
        for r in range(1, N_CHIP):
            piece = pick(pair, r)
            zs[r] = swap(piece, 2 * r)
            pair, piece = lax.optimization_barrier((pair, piece))
        zs[0] = pick(pair, 0)
        left, own, par = [], [], []
        for r in range(N_CHIP):
            a, b = proj_call(zs[r], ms[r], gain[0], bias[0], wt1)
            left.append(a)
            own.append(b)
            par.append(swap(b, 1))
        tri = tri_out_call(pos, left, own, par)
        mids, keeps, recvs = [], [], []
        for r in range(N_CHIP):
            z1, keep, send = mid_call(zs[r], tri[r], ms[r], upd1, (gain[1], bias[1], wt2))
            mids.append(z1)
            keeps.append(keep)
            recvs.append(swap(send, 1))
        t_keep, t_send = tri_in_call(pos, keeps, recvs)
        t_recv = [swap(t, 1) for t in t_send]
        out = None
        for r in range(N_CHIP):
            z2 = last_call(mids[r], t_keep[r], t_recv[r], upd2)
            out = place_call(lax.all_to_all(z2, 'dap', 0, 0, tiled=True), r, out)
        return out.reshape(N_CHIP, -1, *out.shape[3:])

    replicated = P()
    in_specs = (P('data', 'dap', None, None), P('data', 'dap', None), replicated, replicated, replicated,
                replicated, replicated, replicated, replicated)
    return jax.shard_map(body, mesh=mesh, in_specs=in_specs,
                         out_specs=P('data', None, 'dap', None), check_vma=False)
```
